256 devices in a mesh: fsdp: 32 (over z_hi, x, core), tp: 8 (over y, z_lo).
Axes of the slice: x: 4, y: 4, z: 8 (z_hi: 4, z_lo: 2; z = z_hi * 2 + z_lo), core: 2. Of those that a mesh axis runs over, the one named last changes fastest.
Arguments:
- hidden: bfloat16 [8192, 8192], P('fsdp'), may hold values from -6 to 6
- norm_gain: float32 [8192], replicated, may hold values from 0.6 to 6, as said below
- w_query: bfloat16 [8192, 4096], P('fsdp', 'tp'), may hold values from -0.09375 to 0.09375
- w_key: bfloat16 [8192, 512], P('fsdp'), may hold values from -0.09375 to 0.09375
- w_value: bfloat16 [8192, 512], P('fsdp'), may hold values from -0.0625 to 0.0625
- bias_query: bfloat16 [4096], P('tp'), may hold values from -3 to 3
- bias_key: bfloat16 [512], replicated, may hold values from -3 to 3
- bias_value: bfloat16 [512], replicated, may hold values from -3 to 3
- w_out: bfloat16 [4096, 8192], P('tp', 'fsdp'), may hold values from -0.09375 to 0.09375
- seq_lengths: int32 [4], replicated, may hold values from 1 to 6144, 8192 in all
Outputs:
- hidden_out: float32 [8192, 8192], P(('fsdp', 'tp'))
The draws below stay inside these ranges and needn't reach their ends.
Inputs may be any that keep to these rules, and one draw needn't show every extreme that they name: `seq_lengths`: 4 sequences packed in order; the lengths sum to 8192 and the longest has exactly 6144 tokens. `norm_gain`: positive gains.
All inputs are finite; a program needn't handle non-finite values.
Results may differ from the reference program's by a relative error of at most 0.014.
The reference program's roundings to bfloat16 on the way count: a program that leaves them out, or rounds other values in their place, can miss the bound.
Values may be sent and summed in bfloat16 or wider, within the bound.
No kernel may reach another device: no remote copies, remote signals or barrier semaphores. Data moves between devices by JAX's collectives and lax.ppermute only.
A program may use at most 128 MiB of HBM per device.

```python
import math
import jax
import jax.numpy as jnp
import numpy as np
from jax import lax

D = 8192
HEAD = 128
QHEADS = 32
KVHEADS = 4
SEQS = 4
TOKENS = 8192
LONGEST = 6144


def draw_norm_gain(key, part):
    lower, upper = (math.log(0.6), math.log(2.0))
    return jnp.exp(jax.random.uniform(key, (D,), jnp.float32, lower, upper))


def levels(own_key, extent, shards, least, top_value):
    loudness = 1.0
    for axis_at, blocks in shards:
        steps = jax.random.uniform(jax.random.fold_in(jax.random.fold_in(own_key, 6), axis_at), (blocks,), jnp.float32, least / len(shards), top_value / len(shards))
        loudness = loudness * jnp.repeat(jnp.exp(steps), extent[axis_at] // blocks).reshape((-1,) + (1,) * (len(extent) - 1 - axis_at))
    return loudness


def length_profile(number_of, total, bound, slope):
    weights = [(1 << 20) // math.isqrt(standing ** slope) + 1 for standing in range(2, number_of + 1)]
    surplus, holding = total - bound - (number_of - 1), [1] * (number_of - 1)
    while surplus > 0:
        movable = [i for i in range(number_of - 1) if holding[i] < bound]
        whole, left = sum([weights[i] for i in movable]), surplus
        for i in movable:
            more = min(bound - holding[i], max(1, left * weights[i] // whole), surplus)
            holding[i] = holding[i] + more
            surplus = surplus - more
    return np.array([bound] + holding)


def uneven(key, count, total, reach, slope):
    if count == 2:
        one = jax.random.randint(key, (), max(1, total - reach), min(reach, total - 1) + 1)
        return jnp.stack([one, total - one])
    tallies = jnp.asarray(length_profile(count, total, reach, slope), jnp.int32)
    couples = (count - 1) // 2
    donor, taker = tallies[1:1 + 2 * couples:2], tallies[2:2 + 2 * couples:2]
    margin = jnp.minimum(donor - 1, reach - taker)
    moved = jax.random.randint(jax.random.fold_in(key, 1), (couples,), 0, 1 << 20) % (margin + 1)
    tallies = tallies.at[1:1 + 2 * couples:2].set(donor - moved).at[2:2 + 2 * couples:2].set(taker + moved)
    return tallies[jax.random.permutation(jax.random.fold_in(key, 2), count)]


def noise(key, shape, deviation, reach, shards=(), held_as=jnp.bfloat16):
    result = jax.random.normal(key, shape, jnp.float32) * deviation
    if len(shards) > 0:
        result = levels(key, shape, shards, -0.22, 0.18) * result
    return jnp.clip(result, min=-reach, max=reach).astype(held_as)


def setup_inputs(seed: int = 0) -> dict:
    key_list = jax.random.split(jax.random.key(seed), 11)
    return {
        "hidden": noise(key_list[0], (TOKENS, D), 1.0, 6.0, ((0, 32),)),
        "norm_gain": draw_norm_gain(jax.random.fold_in(key_list[10], 71), 0),
        "w_query": noise(key_list[2], (D, QHEADS * HEAD), (1.5 * D ** -0.5), 0.09375, ((0, 32), (1, 8))),
        "w_key": noise(key_list[3], (D, KVHEADS * HEAD), (1.5 * D ** -0.5), 0.09375, ((0, 32),)),
        "w_value": noise(key_list[4], (D, KVHEADS * HEAD), D ** -0.5, 0.0625, ((0, 32),)),
        "bias_query": noise(key_list[5], (QHEADS * HEAD,), 0.5, 3.0, ((0, 8),)),
        "bias_key": noise(key_list[6], (KVHEADS * HEAD,), 0.5, 3.0),
        "bias_value": noise(key_list[7], (KVHEADS * HEAD,), 0.5, 3.0),
        "w_out": noise(key_list[8], (QHEADS * HEAD, D), (QHEADS * HEAD) ** -0.5, 0.09375, ((0, 8), (1, 32))),
        "seq_lengths": uneven(key_list[9], SEQS, TOKENS, LONGEST, 2).astype(jnp.int32),
    }


ROPE_BASE = 1000000.0
EPSILON = 1e-06
FLOOR = -1e+30

def token_layout(seq_lengths, token_index):
    seq_ends = jnp.cumsum(seq_lengths).astype(jnp.int32)
    seq_starts = (seq_ends - seq_lengths).astype(jnp.int32)
    member = (token_index[:, None] >= seq_ends[None, :]).astype(jnp.int32)
    segment = lax.optimization_barrier(jnp.sum(member, axis=1)).astype(jnp.int32)
    one_hot = segment[:, None] == jnp.arange(seq_lengths.shape[0], dtype=jnp.int32)[None, :]
    seq_begin = lax.optimization_barrier(jnp.sum(jnp.where(one_hot, seq_starts[None, :], 0), axis=1)).astype(jnp.int32)
    return (segment, (token_index - seq_begin).astype(jnp.int32))

def rotary(vectors, position):
    half_size = vectors.shape[-1] // 2
    frequency = jnp.exp(jnp.arange(half_size, dtype=jnp.float32) * (-2.0 * math.log(ROPE_BASE) / vectors.shape[-1]))
    angle = position.astype(jnp.float32)[:, None] * frequency[None, :]
    cos_table = jnp.concatenate([jnp.cos(angle), jnp.cos(angle)], axis=1)[:, None, :]
    sin_table = jnp.concatenate([jnp.sin(angle), jnp.sin(angle)], axis=1)[:, None, :]
    turned = jnp.concatenate([-vectors[..., half_size:], vectors[..., :half_size]], axis=-1)
    return vectors * cos_table + turned * sin_table

def rms_normed(hidden, norm_gain):
    widened = hidden.astype(jnp.float32)
    scale = lax.rsqrt(lax.optimization_barrier(jnp.mean(widened * widened, axis=1, keepdims=True)) + EPSILON)
    return (widened * scale * norm_gain.astype(jnp.float32)[None, :]).astype(jnp.bfloat16)

def reference(hidden, norm_gain, w_query, w_key, w_value, bias_query, bias_key, bias_value, w_out, seq_lengths):
    count = hidden.shape[0]
    token_index = jnp.arange(count, dtype=jnp.int32)
    segment, position = token_layout(seq_lengths, token_index)
    normed = rms_normed(hidden, norm_gain)
    query = jnp.dot(normed, w_query, preferred_element_type=jnp.float32) + bias_query.astype(jnp.float32)[None, :]
    keys = jnp.dot(normed, w_key, preferred_element_type=jnp.float32) + bias_key.astype(jnp.float32)[None, :]
    values = jnp.dot(normed, w_value, preferred_element_type=jnp.float32) + bias_value.astype(jnp.float32)[None, :]
    query = rotary(query.reshape(count, QHEADS, HEAD), position).astype(jnp.bfloat16)
    keys = rotary(keys.reshape(count, KVHEADS, HEAD), position).astype(jnp.bfloat16)
    values = values.astype(jnp.bfloat16).reshape(count, KVHEADS, HEAD)
    group = QHEADS // KVHEADS
    block_rows = 256 if count % 256 == 0 else count
    block_count = count // block_rows
    query_blocks = query.reshape(block_count, block_rows, KVHEADS, group, HEAD)
    keys_wide = keys.astype(jnp.float32)
    values_wide = values.astype(jnp.float32)

    def attend_block(query_item):
        query_part, query_segment, query_index = query_item
        scores = jnp.einsum('qkgd,nkd->kgqn', query_part.astype(jnp.float32), keys_wide) * HEAD ** (-0.5)
        allowed = ((query_segment[:, None] == segment[None, :]) & (query_index[:, None] >= token_index[None, :]))[None, None]
        scores = jnp.where(allowed, scores, FLOOR)
        highest = lax.optimization_barrier(jnp.max(scores, axis=3, keepdims=True))
        weights = jnp.where(allowed, jnp.exp(scores - highest), 0.0)
        total = lax.optimization_barrier(jnp.sum(weights, axis=3))
        rounded = weights.astype(jnp.bfloat16).astype(jnp.float32)
        mixed = jnp.einsum('kgqn,nkd->kgqd', rounded, values_wide)
        mixed = mixed / total[..., None]
        return jnp.transpose(mixed, (2, 0, 1, 3)).reshape(block_rows, QHEADS * HEAD)
    attended = lax.map(attend_block, (query_blocks, segment.reshape(block_count, block_rows), token_index.reshape(block_count, block_rows)))
    attended = attended.reshape(count, QHEADS * HEAD).astype(jnp.bfloat16)
    return hidden.astype(jnp.float32) + jnp.dot(attended, w_out, preferred_element_type=jnp.float32)
```

```python
import functools
import math

import jax
import jax.numpy as jnp
from jax import lax
from jax.experimental import pallas as pl
from jax.experimental.pallas import tpu as pltpu
from jax.sharding import Mesh
from jax.sharding import PartitionSpec as P


HEAD = 128
ROPE_BASE = 1000000.0
EPSILON = 1e-06
FLOOR = -1e30
FSDP = ("zh", "x", "co")
TP = ("y", "zl")
ALL = FSDP + TP
BF16 = jnp.bfloat16
F32 = jnp.float32
OFFSETS = (0, -1, 1, 2)


def vmem(count):
    return [pl.BlockSpec(memory_space=pltpu.VMEM)] * count


def smem(count):
    return [pl.BlockSpec(memory_space=pltpu.SMEM)] * count


def call(body, out_shape, ins, scratch=(), smem_count=0, extra=0, flops=0, moved=0, transcendentals=0):
    return pl.pallas_call(
        body,
        out_shape=out_shape,
        in_specs=smem(smem_count) + vmem(len(ins) - smem_count),
        out_specs=pl.BlockSpec(memory_space=pltpu.VMEM),
        scratch_shapes=list(scratch),
        compiler_params=pltpu.CompilerParams(
            vmem_limit_bytes=sum(math.prod(a.shape) * a.dtype.itemsize for a in [*ins, out_shape])
            + extra
            + (4 << 20)
        ),
        cost_estimate=pl.CostEstimate(
            flops=flops, bytes_accessed=moved, transcendentals=transcendentals
        ),
    )(*ins)


def shift(array, axis, by):
    return lax.ppermute(array, axis, [(i, (i + by) % 4) for i in range(4)])


def swap(array, axis):
    return lax.ppermute(array, axis, [(0, 1), (1, 0)])


def around(array, axis):
    return shift(array, axis, 1), shift(array, axis, -1)


def spread(array, axis):
    return [shift(array, axis, -o) for o in OFFSETS[1:]]


def halves(before, after, axis):
    half = before.shape[0] // 2
    return jnp.concatenate([shift(before[:half], axis, 1), shift(after[half:], axis, -1)])


def both_cores(near):
    far = [swap(a, "co") for a in near]
    return [(0, x, 0, a) for x, a in enumerate(near)] + [(1, x, 0, a) for x, a in enumerate(far)]


def ring_gather(array, axis):
    before, after = around(array, axis)
    return [array, before, after, halves(before, after, axis)]


def tp_gather(array):
    other = swap(array, "zl")
    mine, theirs = [array] + spread(array, "y"), [other] + spread(other, "y")
    return [(y, 0, a) for y, a in enumerate(mine)] + [(y, 1, a) for y, a in enumerate(theirs)]


def normalize(hidden_ref, gain_ref, out_ref):
    rows, width = hidden_ref.shape
    span = 256
    chunk = 32

    def step(i, carry):
        at = pl.ds(pl.multiple_of(i * chunk, chunk), chunk)
        total = jnp.zeros((chunk, span), F32)
        for k in range(width // span):
            part = hidden_ref[at, k * span : (k + 1) * span].astype(F32)
            total = total + part * part
        scale = lax.rsqrt(jnp.sum(total, axis=1, keepdims=True) / width + EPSILON)
        for k in range(width // span):
            cols = slice(k * span, (k + 1) * span)
            part = hidden_ref[at, cols].astype(F32)
            out_ref[at, cols] = (part * scale * gain_ref[:, cols]).astype(BF16)
        return carry

    lax.fori_loop(0, rows // chunk, step, 0)


def turn_heads(total, bias_ref, cos_ref, sin_ref, out_ref):
    for h in range(out_ref.shape[1] // HEAD):
        at = slice(h * HEAD, (h + 1) * HEAD)
        u = total[:, at] + bias_ref[:, at]
        out_ref[:, at] = (u * cos_ref[...] + pltpu.roll(u, HEAD // 2, 1) * sin_ref[...]).astype(BF16)


def project_kernel(places, order_ref, hidden_ref, gain_ref, bias_ref, cos_ref, sin_ref, *refs):
    pieces, out_ref, normed_ref = refs[:-2], refs[-2], refs[-1]
    normalize(hidden_ref, gain_ref, normed_ref)
    total = None
    for (core, x, z), piece in zip(places, pieces):
        count, rows, cols = piece.shape
        taken = [order_ref[(core * 4 + x) * 4 + z + k] for k in range(count)]
        part = jnp.dot(
            jnp.concatenate(
                [normed_ref[:, pl.ds(pl.multiple_of(t * rows, rows), rows)] for t in taken], axis=1
            ),
            piece[...].reshape(count * rows, cols),
            preferred_element_type=F32,
        )
        total = part if total is None else total + part
    turn_heads(total, bias_ref, cos_ref, sin_ref, out_ref)


def attend_kernel(places, block_ref, info_ref, query_ref, begin_ref, *refs):
    pieces = refs[: len(places)]
    out_ref, key_ref, value_ref, slot_ref, score_ref, top_ref, sum_ref, mix_ref = refs[len(places) :]
    rows, cols = query_ref.shape
    heads = cols // HEAD
    span = pieces[0].shape[1]
    mine, lowest, full_from = info_ref[0], info_ref[1], info_ref[2]
    last = key_ref.shape[0] - 1
    rate = HEAD**-0.5 * math.log2(math.e)

    def take(slot, number, block):
        key_ref[slot] = block[:, :HEAD]
        value_ref[slot] = block[:, HEAD:].T
        slot_ref[slot] = number

    counts = (jnp.int32(0), jnp.int32(0))
    for (core, x, z), piece in zip(places, pieces):

        def sort(k, counts, piece=piece, base=(core * 4 + x) * 4 + z):
            plain, masked = counts
            number = block_ref[base + k]
            needed = (number <= mine) & (number >= lowest)
            is_plain = needed & (number < mine) & (number >= full_from)
            slot = jnp.where(is_plain, plain, last - masked)
            pl.when(needed)(functools.partial(take, slot, number, piece.at[k]))
            return (
                plain + is_plain.astype(jnp.int32),
                masked + (needed & jnp.logical_not(is_plain)).astype(jnp.int32),
            )

        counts = lax.fori_loop(0, piece.shape[0], sort, counts)
    plain, masked = counts
    odd = plain % 2

    @pl.when(odd == 1)
    def _():
        key_ref[last - masked] = key_ref[plain - 1]
        value_ref[last - masked] = value_ref[plain - 1]
        slot_ref[last - masked] = slot_ref[plain - 1]

    plain, masked = plain - odd, masked + odd

    @pl.when(masked % 2 == 1)
    def _():
        take(last - masked, jnp.int32(1 << 20), pieces[0].at[0])

    top_ref[...] = jnp.full(top_ref.shape, FLOOR, F32)
    sum_ref[...] = jnp.zeros(sum_ref.shape, F32)
    mix_ref[...] = jnp.zeros(mix_ref.shape, F32)

    def fold(slots, allowed):
        def score(h):
            for i, slot in enumerate(slots):
                score_ref[h % 2, i * span : (i + 1) * span] = lax.dot_general(
                    key_ref[slot],
                    query_ref[:, h * HEAD : (h + 1) * HEAD],
                    (((1,), (1,)), ((), ())),
                    preferred_element_type=F32,
                )

        score(0)
        for h in range(heads):
            if h + 1 < heads:
                score(h + 1)
            at = slice(h * rows, (h + 1) * rows)
            scores = score_ref[h % 2]
            if allowed is not None:
                scores = jnp.where(allowed, scores, FLOOR)
            old = top_ref[:, at]
            new = jnp.maximum(old, jnp.max(scores, axis=0, keepdims=True))
            weights = jnp.exp2((scores - new) * rate)
            factor = jnp.exp2((old - new) * rate)
            top_ref[:, at] = new
            sum_ref[:, at] = sum_ref[:, at] * factor + jnp.sum(weights, axis=0, keepdims=True)
            mix_ref[:, at] = mix_ref[:, at] * factor + jnp.dot(
                jnp.concatenate([value_ref[slot] for slot in slots], axis=1),
                weights.astype(BF16),
                preferred_element_type=F32,
            )

    def masked_step(i, carry):
        slots = (last - 2 * i, last - 2 * i - 1)
        place = lax.broadcasted_iota(jnp.int32, (span, rows), 0)
        key_at = jnp.concatenate([slot_ref[slot] * span + place for slot in slots], axis=0)
        query_at = mine * rows + lax.broadcasted_iota(jnp.int32, (2 * span, rows), 1)
        fold(slots, (key_at <= query_at) & (key_at >= begin_ref[...]))
        return carry

    def plain_step(i, carry):
        fold((2 * i, 2 * i + 1), None)
        return carry

    lax.fori_loop(0, (masked + 1) // 2, masked_step, 0)
    lax.fori_loop(0, plain // 2, plain_step, 0)
    for h in range(heads):
        at = slice(h * rows, (h + 1) * rows)
        out_ref[:, h * HEAD : (h + 1) * HEAD] = (mix_ref[:, at] / sum_ref[:, at]).T.astype(BF16)


def output_kernel(places, att_places, row_ref, col_ref, tp_ref, *refs):
    pieces = refs[: len(places)]
    parts = refs[len(places) : len(places) + len(att_places)]
    out_ref, att_ref = refs[len(places) + len(att_places) :]
    for (y, zl), part in zip(att_places, parts):
        att_ref[tp_ref[y * 2 + zl]] = part[...]
    count, _, width = pieces[0].shape
    for k in range(count):
        total = None
        for (core, x), piece in zip(places, pieces):
            part = jnp.dot(
                att_ref[row_ref[core * 4 + x]], piece[k], preferred_element_type=F32
            )
            total = part if total is None else total + part
        col = pl.ds(pl.multiple_of(col_ref[k] * width, width), width)
        out_ref[:, col] = total.astype(BF16)


def shards(hidden, norm_gain, w_query, w_key, w_value, bias_query, bias_key, bias_value, w_out, seq_lengths):
    rows, width = hidden.shape
    zh, x, co, y, zl = (lax.axis_index(a) for a in ALL)
    mine = (zh * 4 + x) * 2 + co
    off = jnp.array([o % 4 for o in OFFSETS], jnp.int32)
    src_z, src_x = (zh + off) % 4, (x + off) % 4
    src_c = jnp.stack([co, 1 - co])
    order = (
        src_z[None, None, :] * 8 + src_x[None, :, None] * 2 + src_c[:, None, None]
    ).reshape(32).astype(jnp.int32)

    moves = []
    for d in range(256):
        l = d % 2
        yy = d // 2 % 4
        c = d // 8 % 2
        xx = d // 16 % 4
        zz = d // 64
        moves.append((d, (((zz * 4 + (xx + yy) % 4) * 2 + l) * 4 + xx) * 2 + c))
    pick_key = zl == 0
    at = y * HEAD
    kv_block = jnp.where(
        pick_key,
        lax.dynamic_slice_in_dim(w_key, at, HEAD, 1),
        lax.dynamic_slice_in_dim(w_value, at, HEAD, 1),
    )
    kv_bias = jnp.where(
        pick_key,
        lax.dynamic_slice_in_dim(bias_key, at, HEAD, 0),
        lax.dynamic_slice_in_dim(bias_value, at, HEAD, 0),
    )
    kv_stack = jnp.stack([kv_block] + spread(kv_block, "zh"))
    kv_weights = both_cores([kv_stack] + spread(kv_stack, "x"))
    q_stack = jnp.stack(ring_gather(w_query, "zh"))
    q_weights = both_cores(ring_gather(q_stack, "x"))
    out_block = lax.ppermute(w_out, ALL, moves)
    out_stack = jnp.stack(ring_gather(out_block, "zh"))
    out_weights = both_cores(ring_gather(out_stack, "x"))

    ends = jnp.cumsum(seq_lengths)
    index = mine * rows + jnp.arange(rows, dtype=jnp.int32)
    begin = jnp.max(jnp.where(index[:, None] >= ends[None, :], ends[None, :], 0), axis=1).astype(jnp.int32)
    position = (index - begin).astype(F32)
    frequency = jnp.exp(jnp.arange(HEAD // 2, dtype=F32) * (-2.0 * math.log(ROPE_BASE) / HEAD))
    angle = position[:, None] * frequency[None, :]
    cos, sin = jnp.cos(angle), jnp.sin(angle)
    cos = jnp.concatenate([cos, cos], axis=1)
    sin = jnp.concatenate([-sin, sin], axis=1)
    kv_cos = jnp.where(pick_key, cos, 1.0)
    kv_sin = jnp.where(pick_key, sin, 0.0)

    def project(pieces, bias, cos, sin):
        cols = bias.shape[0]
        return call(
            functools.partial(project_kernel, [p[:3] for p in pieces]),
            jax.ShapeDtypeStruct((rows, cols), BF16),
            (
                order,
                hidden,
                norm_gain[None, :],
                bias.astype(F32)[None, :],
                cos,
                sin,
                *[p[3] for p in pieces],
            ),
            scratch=[pltpu.VMEM((rows, width), BF16)],
            smem_count=1,
            extra=rows * width * 2,
            flops=2 * rows * width * cols,
            moved=2 * width * (rows + cols),
        )

    kv_own = project(kv_weights, kv_bias, kv_cos, kv_sin)
    kv_other = swap(kv_own, "zl")
    kv_pair = jnp.concatenate(
        [jnp.where(pick_key, kv_own, kv_other), jnp.where(pick_key, kv_other, kv_own)], axis=1
    )
    kv_stack = jnp.stack([kv_pair] + spread(kv_pair, "zh"))
    kv = both_cores(ring_gather(kv_stack, "x"))
    query = project(q_weights, bias_query, cos, sin)
    info = jnp.stack([mine, begin[0] // rows, (begin[rows - 1] + rows - 1) // rows]).astype(jnp.int32)
    heads = query.shape[1] // HEAD
    attended = call(
        functools.partial(attend_kernel, [p[:3] for p in kv]),
        jax.ShapeDtypeStruct(query.shape, BF16),
        (order, info, query, begin[None, :], *[p[3] for p in kv]),
        scratch=[
            pltpu.VMEM((34, rows, HEAD), BF16),
            pltpu.VMEM((34, HEAD, rows), BF16),
            pltpu.SMEM((34,), jnp.int32),
            pltpu.VMEM((2, 2 * rows, rows), F32),
            pltpu.VMEM((1, heads * rows), F32),
            pltpu.VMEM((1, heads * rows), F32),
            pltpu.VMEM((HEAD, heads * rows), F32),
        ],
        smem_count=2,
        extra=10 << 20,
        flops=4 * heads * rows * 6144 * HEAD * 2,
        moved=5 * 1024 * 1024,
        transcendentals=heads * rows * 6144,
    )

    parts = tp_gather(attended)
    row_of = (((src_x - y) % 4)[None, :] * 2 + src_c[:, None]).reshape(8).astype(jnp.int32)
    tp_of = (
        ((y + off) % 4)[:, None] * 2 + jnp.stack([zl, 1 - zl])[None, :]
    ).reshape(8).astype(jnp.int32)
    cols = width // 8
    mixed = call(
        functools.partial(output_kernel, [p[:2] for p in out_weights], [p[:2] for p in parts]),
        jax.ShapeDtypeStruct((rows, cols), BF16),
        (row_of, src_z.astype(jnp.int32), tp_of, *[p[3] for p in out_weights], *[p[2] for p in parts]),
        scratch=[pltpu.VMEM((8,) + query.shape, BF16)],
        smem_count=3,
        extra=4 << 20,
        flops=2 * rows * cols * 4096,
        moved=12 * 1024 * 1024,
    )
    share = rows // 8
    landed = lax.all_to_all(mixed.reshape(8, share, cols), TP, 0, 0, tiled=True)
    own = lax.dynamic_slice_in_dim(hidden, (y * 2 + zl) * share, share, 0).astype(F32)
    landed = jnp.transpose(landed.reshape(8, share, 4, cols // 4), (1, 2, 0, 3))
    return own + landed.reshape(share, width).astype(F32)


def solution(mesh):
    fine = Mesh(mesh.devices.reshape(4, 4, 2, 4, 2), ALL)

    return jax.shard_map(
        shards,
        mesh=fine,
        in_specs=(
            P(FSDP, None),
            P(),
            P(FSDP, TP),
            P(FSDP, None),
            P(FSDP, None),
            P(TP),
            P(),
            P(),
            P(TP, FSDP),
            P(),
        ),
        out_specs=P(ALL, None),
        check_vma=False,
    )
```

```python
import functools
import math

import jax
import jax.numpy as jnp
from jax import lax
from jax.experimental import pallas as pl
from jax.experimental.pallas import tpu as pltpu
from jax.sharding import Mesh
from jax.sharding import PartitionSpec as P


HEAD = 128
ROPE_BASE = 1000000.0
EPSILON = 1e-06
FLOOR = -1e30
FSDP = ("zh", "x", "co")
TP = ("y", "zl")
ALL = FSDP + TP
BF16 = jnp.bfloat16
F32 = jnp.float32
OFFSETS = (0, -1, 1, 2)


def vmem(count):
    return [pl.BlockSpec(memory_space=pltpu.VMEM)] * count


def smem(count):
    return [pl.BlockSpec(memory_space=pltpu.SMEM)] * count


def call(body, out_shape, ins, scratch=(), smem_count=0, extra=0, flops=0, moved=0, transcendentals=0):
    return pl.pallas_call(
        body,
        out_shape=out_shape,
        in_specs=smem(smem_count) + vmem(len(ins) - smem_count),
        out_specs=pl.BlockSpec(memory_space=pltpu.VMEM),
        scratch_shapes=list(scratch),
        compiler_params=pltpu.CompilerParams(
            vmem_limit_bytes=sum(math.prod(a.shape) * a.dtype.itemsize for a in [*ins, out_shape])
            + extra
            + (4 << 20)
        ),
        cost_estimate=pl.CostEstimate(
            flops=flops, bytes_accessed=moved, transcendentals=transcendentals
        ),
    )(*ins)


def shift(array, axis, by):
    return lax.ppermute(array, axis, [(i, (i + by) % 4) for i in range(4)])


def swap(array, axis):
    return lax.ppermute(array, axis, [(0, 1), (1, 0)])


def around(array, axis):
    return shift(array, axis, 1), shift(array, axis, -1)


def spread(array, axes, count):
    copies = jnp.broadcast_to(array[None], (count,) + array.shape)
    return lax.all_to_all(copies, axes, 0, 0, tiled=True)


def halves(before, after, axis):
    half = before.shape[0] // 2
    return jnp.concatenate([shift(before[:half], axis, 1), shift(after[half:], axis, -1)])


def both_cores(near):
    far = [swap(a, "co") for a in near]
    return [(0, x, 0, a) for x, a in enumerate(near)] + [(1, x, 0, a) for x, a in enumerate(far)]


def ring_gather(array, axis):
    before, after = around(array, axis)
    return [array, before, after, halves(before, after, axis)]


def normalize(hidden_ref, gain_ref, out_ref):
    rows, width = hidden_ref.shape
    span = 256
    chunk = 32

    def step(i, carry):
        at = pl.ds(pl.multiple_of(i * chunk, chunk), chunk)
        total = jnp.zeros((chunk, span), F32)
        for k in range(width // span):
            part = hidden_ref[at, k * span : (k + 1) * span].astype(F32)
            total = total + part * part
        scale = lax.rsqrt(jnp.sum(total, axis=1, keepdims=True) / width + EPSILON)
        for k in range(width // span):
            cols = slice(k * span, (k + 1) * span)
            part = hidden_ref[at, cols].astype(F32)
            out_ref[at, cols] = (part * scale * gain_ref[:, cols]).astype(BF16)
        return carry

    lax.fori_loop(0, rows // chunk, step, 0)


def turn_heads(total, bias_ref, cos_ref, sin_ref, out_ref):
    for h in range(out_ref.shape[1] // HEAD):
        at = slice(h * HEAD, (h + 1) * HEAD)
        u = total[:, at] + bias_ref[:, at]
        out_ref[:, at] = (u * cos_ref[...] + pltpu.roll(u, HEAD // 2, 1) * sin_ref[...]).astype(BF16)


def project_kernel(places, order_ref, hidden_ref, gain_ref, bias_ref, cos_ref, sin_ref, *refs):
    pieces, out_ref, normed_ref = refs[:-2], refs[-2], refs[-1]
    normalize(hidden_ref, gain_ref, normed_ref)
    total = None
    group = 4
    for (core, x, z), piece in zip(places, pieces):
        count, rows, cols = piece.shape
        for k in range(0, count, group):
            taken = [order_ref[(core * 4 + x) * 4 + z + k + i] for i in range(group)]
            part = jnp.dot(
                jnp.concatenate(
                    [normed_ref[:, pl.ds(pl.multiple_of(t * rows, rows), rows)] for t in taken], axis=1
                ),
                piece[k : k + group].reshape(group * rows, cols),
                preferred_element_type=F32,
            )
            total = part if total is None else total + part
    turn_heads(total, bias_ref, cos_ref, sin_ref, out_ref)


def attend_kernel(places, block_ref, info_ref, query_ref, begin_ref, *refs):
    pieces = refs[: len(places)]
    out_ref, key_ref, value_ref, slot_ref, score_ref, top_ref, sum_ref, mix_ref = refs[len(places) :]
    rows, cols = query_ref.shape
    heads = cols // HEAD
    span = pieces[0].shape[1]
    mine, lowest, full_from = info_ref[0], info_ref[1], info_ref[2]
    last = key_ref.shape[0] - 1
    rate = HEAD**-0.5 * math.log2(math.e)

    def take(slot, number, block):
        key_ref[slot] = block[:, :HEAD]
        value_ref[slot] = block[:, HEAD:].T
        slot_ref[slot] = number

    counts = (jnp.int32(0), jnp.int32(0))
    for (core, x, z), piece in zip(places, pieces):

        def sort(k, counts, piece=piece, base=(core * 4 + x) * 4 + z):
            plain, masked = counts
            number = block_ref[base + k]
            needed = (number <= mine) & (number >= lowest)
            is_plain = needed & (number < mine) & (number >= full_from)
            slot = jnp.where(is_plain, plain, last - masked)
            pl.when(needed)(functools.partial(take, slot, number, piece.at[k]))
            return (
                plain + is_plain.astype(jnp.int32),
                masked + (needed & jnp.logical_not(is_plain)).astype(jnp.int32),
            )

        counts = lax.fori_loop(0, piece.shape[0], sort, counts)
    plain, masked = counts
    odd = plain % 2

    @pl.when(odd == 1)
    def _():
        key_ref[last - masked] = key_ref[plain - 1]
        value_ref[last - masked] = value_ref[plain - 1]
        slot_ref[last - masked] = slot_ref[plain - 1]

    plain, masked = plain - odd, masked + odd

    @pl.when(masked % 2 == 1)
    def _():
        take(last - masked, jnp.int32(1 << 20), pieces[0].at[0])

    top_ref[...] = jnp.full(top_ref.shape, FLOOR, F32)
    sum_ref[...] = jnp.zeros(sum_ref.shape, F32)
    mix_ref[...] = jnp.zeros(mix_ref.shape, F32)

    def fold(slots, allowed):
        def score(h):
            for i, slot in enumerate(slots):
                score_ref[h % 2, i * span : (i + 1) * span] = lax.dot_general(
                    key_ref[slot],
                    query_ref[:, h * HEAD : (h + 1) * HEAD],
                    (((1,), (1,)), ((), ())),
                    preferred_element_type=F32,
                )

        score(0)
        for h in range(heads):
            if h + 1 < heads:
                score(h + 1)
            at = slice(h * rows, (h + 1) * rows)
            scores = score_ref[h % 2]
            if allowed is not None:
                scores = jnp.where(allowed, scores, FLOOR)
            old = top_ref[:, at]
            new = jnp.maximum(old, jnp.max(scores, axis=0, keepdims=True))
            weights = jnp.exp2((scores - new) * rate)
            factor = jnp.exp2((old - new) * rate)
            top_ref[:, at] = new
            sum_ref[:, at] = sum_ref[:, at] * factor + jnp.sum(weights, axis=0, keepdims=True)
            mix_ref[:, at] = mix_ref[:, at] * factor + jnp.dot(
                jnp.concatenate([value_ref[slot] for slot in slots], axis=1),
                weights.astype(BF16),
                preferred_element_type=F32,
            )

    def masked_step(i, carry):
        slots = (last - 2 * i, last - 2 * i - 1)
        place = lax.broadcasted_iota(jnp.int32, (span, rows), 0)
        key_at = jnp.concatenate([slot_ref[slot] * span + place for slot in slots], axis=0)
        query_at = mine * rows + lax.broadcasted_iota(jnp.int32, (2 * span, rows), 1)
        fold(slots, (key_at <= query_at) & (key_at >= begin_ref[...]))
        return carry

    def plain_step(i, carry):
        fold((2 * i, 2 * i + 1), None)
        return carry

    lax.fori_loop(0, (masked + 1) // 2, masked_step, 0)
    lax.fori_loop(0, plain // 2, plain_step, 0)
    for h in range(heads):
        at = slice(h * rows, (h + 1) * rows)
        out_ref[:, h * HEAD : (h + 1) * HEAD] = (mix_ref[:, at] / sum_ref[:, at]).T.astype(BF16)


def output_kernel(places, row_ref, col_ref, att_ref, *refs):
    pieces, out_ref = refs[:-1], refs[-1]
    count, _, width = pieces[0].shape
    for k in range(count):
        total = None
        for (core, x), piece in zip(places, pieces):
            part = jnp.dot(
                att_ref[row_ref[core * 4 + x]], piece[k], preferred_element_type=F32
            )
            total = part if total is None else total + part
        col = pl.ds(pl.multiple_of(col_ref[k] * width, width), width)
        out_ref[:, col] = total.astype(BF16)


def row_kernel(in_ref, out_ref):
    out_ref[...] = in_ref[...]


def finish_kernel(hidden_ref, landed_ref, out_ref):
    count, _, cols = landed_ref.shape
    width = cols // 4
    for j in range(4):
        for c in range(count):
            at = slice((j * count + c) * width, (j * count + c + 1) * width)
            part = landed_ref[c, :, j * width : (j + 1) * width]
            out_ref[:, at] = hidden_ref[:, at].astype(F32) + part.astype(F32)


def shards(hidden, norm_gain, w_query, w_key, w_value, bias_query, bias_key, bias_value, w_out, seq_lengths):
    rows, width = hidden.shape
    zh, x, co, y, zl = (lax.axis_index(a) for a in ALL)
    mine = (zh * 4 + x) * 2 + co
    off = jnp.array([o % 4 for o in OFFSETS], jnp.int32)
    src_z, src_x = (zh + off) % 4, (x + off) % 4
    src_c = jnp.stack([co, 1 - co])
    all_4 = jnp.arange(4, dtype=jnp.int32)

    def table(x_at, z_at):
        places = z_at[None, None, :] * 8 + x_at[None, :, None] * 2 + src_c[:, None, None]
        return places.reshape(32).astype(jnp.int32)

    q_order, kv_order, block_order = table(src_x, src_z), table(all_4, all_4), table(src_x, all_4)

    moves = []
    for d in range(256):
        l = d % 2
        yy = d // 2 % 4
        c = d // 8 % 2
        xx = d // 16 % 4
        zz = d // 64
        moves.append((d, (((zz * 4 + (xx + yy) % 4) * 2 + l) * 4 + xx) * 2 + c))
    pick_key = zl == 0
    at = y * HEAD
    kv_block = jnp.where(
        pick_key,
        lax.dynamic_slice_in_dim(w_key, at, HEAD, 1),
        lax.dynamic_slice_in_dim(w_value, at, HEAD, 1),
    )
    kv_bias = jnp.where(
        pick_key,
        lax.dynamic_slice_in_dim(bias_key, at, HEAD, 0),
        lax.dynamic_slice_in_dim(bias_value, at, HEAD, 0),
    )
    kv_stack = spread(spread(kv_block, "zh", 4), "x", 4).reshape(16, -1, HEAD)
    kv_weights = both_cores([kv_stack])
    q_stack = jnp.stack(ring_gather(w_query, "zh"))
    q_weights = both_cores(ring_gather(q_stack, "x"))
    out_block = lax.ppermute(w_out, ALL, moves)
    out_stack = jnp.stack(ring_gather(out_block, "zh"))
    out_weights = both_cores(ring_gather(out_stack, "x"))

    ends = jnp.cumsum(seq_lengths)
    index = mine * rows + jnp.arange(rows, dtype=jnp.int32)
    begin = jnp.max(jnp.where(index[:, None] >= ends[None, :], ends[None, :], 0), axis=1).astype(jnp.int32)
    position = (index - begin).astype(F32)
    frequency = jnp.exp(jnp.arange(HEAD // 2, dtype=F32) * (-2.0 * math.log(ROPE_BASE) / HEAD))
    angle = position[:, None] * frequency[None, :]
    cos, sin = jnp.cos(angle), jnp.sin(angle)
    cos = jnp.concatenate([cos, cos], axis=1)
    sin = jnp.concatenate([-sin, sin], axis=1)
    kv_cos = jnp.where(pick_key, cos, 1.0)
    kv_sin = jnp.where(pick_key, sin, 0.0)

    def project(pieces, order, bias, cos, sin):
        cols = bias.shape[0]
        return call(
            functools.partial(project_kernel, [p[:3] for p in pieces]),
            jax.ShapeDtypeStruct((rows, cols), BF16),
            (
                order,
                hidden,
                norm_gain[None, :],
                bias.astype(F32)[None, :],
                cos,
                sin,
                *[p[3] for p in pieces],
            ),
            scratch=[pltpu.VMEM((rows, width), BF16)],
            smem_count=1,
            extra=rows * width * 2,
            flops=2 * rows * width * cols,
            moved=2 * width * (rows + cols),
        )

    kv_own = project(kv_weights, kv_order, kv_bias, kv_cos, kv_sin)
    kv_other = swap(kv_own, "zl")
    kv_pair = jnp.concatenate(
        [jnp.where(pick_key, kv_own, kv_other), jnp.where(pick_key, kv_other, kv_own)], axis=1
    )
    kv_stack = spread(kv_pair, "zh", 4)
    kv = both_cores(ring_gather(kv_stack, "x"))
    query = project(q_weights, q_order, bias_query, cos, sin)
    begin_row = call(row_kernel, jax.ShapeDtypeStruct((1, rows), jnp.int32), (begin[None, :],))
    info = jnp.stack([mine, begin[0] // rows, (begin[rows - 1] + rows - 1) // rows]).astype(jnp.int32)
    heads = query.shape[1] // HEAD
    attended = call(
        functools.partial(attend_kernel, [p[:3] for p in kv]),
        jax.ShapeDtypeStruct(query.shape, BF16),
        (block_order, info, query, begin_row, *[p[3] for p in kv]),
        scratch=[
            pltpu.VMEM((34, rows, HEAD), BF16),
            pltpu.VMEM((34, HEAD, rows), BF16),
            pltpu.SMEM((34,), jnp.int32),
            pltpu.VMEM((2, 2 * rows, rows), F32),
            pltpu.VMEM((1, heads * rows), F32),
            pltpu.VMEM((1, heads * rows), F32),
            pltpu.VMEM((HEAD, heads * rows), F32),
        ],
        smem_count=2,
        extra=10 << 20,
        flops=4 * heads * rows * 6144 * HEAD * 2,
        moved=5 * 1024 * 1024,
        transcendentals=heads * rows * 6144,
    )

    parts = spread(attended, TP, 8)
    row_of = (((src_x - y) % 4)[None, :] * 2 + src_c[:, None]).reshape(8).astype(jnp.int32)
    cols = width // 8
    mixed = call(
        functools.partial(output_kernel, [p[:2] for p in out_weights]),
        jax.ShapeDtypeStruct((rows, cols), BF16),
        (row_of, src_z.astype(jnp.int32), parts, *[p[3] for p in out_weights]),
        smem_count=2,
        flops=2 * rows * cols * 4096,
        moved=12 * 1024 * 1024,
    )
    share = rows // 8
    landed = lax.all_to_all(mixed.reshape(8, share, cols), TP, 0, 0, tiled=True)
    own = lax.dynamic_slice_in_dim(hidden, (y * 2 + zl) * share, share, 0)
    return call(
        finish_kernel,
        jax.ShapeDtypeStruct((share, width), F32),
        (own, landed),
        flops=2 * share * width,
        moved=8 * share * width,
    )


def solution(mesh):
    fine = Mesh(mesh.devices.reshape(4, 4, 2, 4, 2), ALL)

    return jax.shard_map(
        shards,
        mesh=fine,
        in_specs=(
            P(FSDP, None),
            P(),
            P(FSDP, TP),
            P(FSDP, None),
            P(FSDP, None),
            P(TP),
            P(),
            P(),
            P(TP, FSDP),
            P(),
        ),
        out_specs=P(ALL, None),
        check_vma=False,
    )
```

```python
import functools
import math

import jax
import jax.numpy as jnp
from jax import lax
from jax.experimental import pallas as pl
from jax.experimental.pallas import tpu as pltpu
from jax.sharding import Mesh
from jax.sharding import PartitionSpec as P


HEAD = 128
ROPE_BASE = 1000000.0
EPSILON = 1e-06
FLOOR = -1e30
FSDP = ("zh", "x", "co")
TP = ("y", "zl")
ALL = FSDP + TP
BF16 = jnp.bfloat16
F32 = jnp.float32
OFFSETS = (0, -1, 1, 2)

Q_ORDER, ROWS, COLS, INFO = 32, 64, 72, 76


def vmem(count):
    return [pl.BlockSpec(memory_space=pltpu.VMEM)] * count


def smem(count):
    return [pl.BlockSpec(memory_space=pltpu.SMEM)] * count


def call(body, out_shape, ins, scratch=(), smem_count=0, extra=0, flops=0, moved=0, transcendentals=0):
    return pl.pallas_call(
        body,
        out_shape=out_shape,
        in_specs=smem(smem_count) + vmem(len(ins) - smem_count),
        out_specs=pl.BlockSpec(memory_space=pltpu.VMEM),
        scratch_shapes=list(scratch),
        compiler_params=pltpu.CompilerParams(
            vmem_limit_bytes=sum(math.prod(a.shape) * a.dtype.itemsize for a in [*ins, out_shape])
            + extra
            + (4 << 20)
        ),
        cost_estimate=pl.CostEstimate(
            flops=flops, bytes_accessed=moved, transcendentals=transcendentals
        ),
    )(*ins)


def shift(array, axis, by):
    return lax.ppermute(array, axis, [(i, (i + by) % 4) for i in range(4)])


def swap(array, axis):
    return lax.ppermute(array, axis, [(0, 1), (1, 0)])


def around(array, axis):
    return shift(array, axis, 1), shift(array, axis, -1)


def spread(array, axes, count):
    copies = jnp.broadcast_to(array[None], (count,) + array.shape)
    return lax.all_to_all(copies, axes, 0, 0, tiled=True)


def halves(before, after, axis):
    half = before.shape[0] // 2
    return jnp.concatenate([shift(before[:half], axis, 1), shift(after[half:], axis, -1)])


def both_cores(near):
    far = [swap(a, "co") for a in near]
    return [(0, x, 0, a) for x, a in enumerate(near)] + [(1, x, 0, a) for x, a in enumerate(far)]


def ring_gather(array, axis):
    before, after = around(array, axis)
    return [array, before, after, halves(before, after, axis)]


def normalize(hidden_ref, gain_ref, out_ref):
    rows, width = hidden_ref.shape
    span = 256
    chunk = 32

    def step(i, carry):
        at = pl.ds(pl.multiple_of(i * chunk, chunk), chunk)
        total = jnp.zeros((chunk, span), F32)
        for k in range(width // span):
            part = hidden_ref[at, k * span : (k + 1) * span].astype(F32)
            total = total + part * part
        scale = lax.rsqrt(jnp.sum(total, axis=1, keepdims=True) / width + EPSILON)
        for k in range(width // span):
            cols = slice(k * span, (k + 1) * span)
            part = hidden_ref[at, cols].astype(F32)
            out_ref[at, cols] = (part * scale * gain_ref[:, cols]).astype(BF16)
        return carry

    lax.fori_loop(0, rows // chunk, step, 0)


def turn_heads(total, bias_ref, cos_ref, sin_ref, out_ref):
    for h in range(out_ref.shape[1] // HEAD):
        at = slice(h * HEAD, (h + 1) * HEAD)
        u = total[:, at] + bias_ref[:, at]
        out_ref[:, at] = (u * cos_ref[...] + pltpu.roll(u, HEAD // 2, 1) * sin_ref[...]).astype(BF16)


def project_kernel(places, base, order_ref, hidden_ref, gain_ref, bias_ref, cos_ref, sin_ref, *refs):
    pieces, out_ref, normed_ref = refs[:-2], refs[-2], refs[-1]
    normalize(hidden_ref, gain_ref, normed_ref)
    total = None
    group = 4
    for (core, x, z), piece in zip(places, pieces):
        count, rows, cols = piece.shape
        for k in range(0, count, group):
            taken = [order_ref[base + (core * 4 + x) * 4 + z + k + i] for i in range(group)]
            part = jnp.dot(
                jnp.concatenate(
                    [normed_ref[:, pl.ds(pl.multiple_of(t * rows, rows), rows)] for t in taken], axis=1
                ),
                piece[k : k + group].reshape(group * rows, cols),
                preferred_element_type=F32,
            )
            total = part if total is None else total + part
    turn_heads(total, bias_ref, cos_ref, sin_ref, out_ref)


def attend_kernel(places, block_ref, query_ref, begin_ref, *refs):
    pieces = refs[: len(places)]
    out_ref, key_ref, value_ref, slot_ref, score_ref, top_ref, sum_ref, mix_ref = refs[len(places) :]
    rows, cols = query_ref.shape
    heads = cols // HEAD
    span = pieces[0].shape[1]
    mine, lowest, full_from = (block_ref[INFO + k] for k in range(3))
    last = key_ref.shape[0] - 1
    rate = HEAD**-0.5 * math.log2(math.e)

    def take(slot, number, block):
        key_ref[slot] = block[:, :HEAD]
        value_ref[slot] = block[:, HEAD:].T
        slot_ref[slot] = number

    counts = (jnp.int32(0), jnp.int32(0))
    for (core, x, z), piece in zip(places, pieces):

        def sort(k, counts, piece=piece, base=(core * 4 + x) * 4 + z):
            plain, masked = counts
            number = block_ref[base + k]
            needed = (number <= mine) & (number >= lowest)
            is_plain = needed & (number < mine) & (number >= full_from)
            slot = jnp.where(is_plain, plain, last - masked)
            pl.when(needed)(functools.partial(take, slot, number, piece.at[k]))
            return (
                plain + is_plain.astype(jnp.int32),
                masked + (needed & jnp.logical_not(is_plain)).astype(jnp.int32),
            )

        counts = lax.fori_loop(0, piece.shape[0], sort, counts)
    plain, masked = counts
    odd = plain % 2

    @pl.when(odd == 1)
    def _():
        key_ref[last - masked] = key_ref[plain - 1]
        value_ref[last - masked] = value_ref[plain - 1]
        slot_ref[last - masked] = slot_ref[plain - 1]

    plain, masked = plain - odd, masked + odd

    @pl.when(masked % 2 == 1)
    def _():
        take(last - masked, jnp.int32(1 << 20), pieces[0].at[0])

    top_ref[...] = jnp.full(top_ref.shape, FLOOR, F32)
    sum_ref[...] = jnp.zeros(sum_ref.shape, F32)
    mix_ref[...] = jnp.zeros(mix_ref.shape, F32)

    def fold(slots, allowed):
        def score(h):
            for i, slot in enumerate(slots):
                score_ref[h % 2, i * span : (i + 1) * span] = lax.dot_general(
                    key_ref[slot],
                    query_ref[:, h * HEAD : (h + 1) * HEAD],
                    (((1,), (1,)), ((), ())),
                    preferred_element_type=F32,
                )

        score(0)
        for h in range(heads):
            if h + 1 < heads:
                score(h + 1)
            at = slice(h * rows, (h + 1) * rows)
            scores = score_ref[h % 2]
            if allowed is not None:
                scores = jnp.where(allowed, scores, FLOOR)
            old = top_ref[:, at]
            new = jnp.maximum(old, jnp.max(scores, axis=0, keepdims=True))
            weights = jnp.exp2((scores - new) * rate)
            factor = jnp.exp2((old - new) * rate)
            top_ref[:, at] = new
            sum_ref[:, at] = sum_ref[:, at] * factor + jnp.sum(weights, axis=0, keepdims=True)
            mix_ref[:, at] = mix_ref[:, at] * factor + jnp.dot(
                jnp.concatenate([value_ref[slot] for slot in slots], axis=1),
                weights.astype(BF16),
                preferred_element_type=F32,
            )

    def masked_step(i, carry):
        slots = (last - 2 * i, last - 2 * i - 1)
        place = lax.broadcasted_iota(jnp.int32, (span, rows), 0)
        key_at = jnp.concatenate([slot_ref[slot] * span + place for slot in slots], axis=0)
        query_at = mine * rows + lax.broadcasted_iota(jnp.int32, (2 * span, rows), 1)
        fold(slots, (key_at <= query_at) & (key_at >= begin_ref[...]))
        return carry

    def plain_step(i, carry):
        fold((2 * i, 2 * i + 1), None)
        return carry

    lax.fori_loop(0, (masked + 1) // 2, masked_step, 0)
    lax.fori_loop(0, plain // 2, plain_step, 0)
    for h in range(heads):
        at = slice(h * rows, (h + 1) * rows)
        out_ref[:, h * HEAD : (h + 1) * HEAD] = (mix_ref[:, at] / sum_ref[:, at]).T.astype(BF16)


def output_kernel(places, row_ref, att_ref, *refs):
    pieces, out_ref = refs[:-1], refs[-1]
    count, _, width = pieces[0].shape
    for k in range(count):
        total = None
        for (core, x), piece in zip(places, pieces):
            part = jnp.dot(
                att_ref[row_ref[ROWS + core * 4 + x]], piece[k], preferred_element_type=F32
            )
            total = part if total is None else total + part
        col = pl.ds(pl.multiple_of(row_ref[COLS + k] * width, width), width)
        out_ref[:, col] = total.astype(BF16)


def row_kernel(in_ref, out_ref):
    for k in range(in_ref.shape[0]):
        out_ref[k] = in_ref[k]


def finish_kernel(hidden_ref, landed_ref, out_ref):
    count, _, cols = landed_ref.shape
    width = cols // 4
    for j in range(4):
        for c in range(count):
            at = slice((j * count + c) * width, (j * count + c + 1) * width)
            part = landed_ref[c, :, j * width : (j + 1) * width]
            out_ref[:, at] = hidden_ref[:, at].astype(F32) + part.astype(F32)


def shards(hidden, norm_gain, w_query, w_key, w_value, bias_query, bias_key, bias_value, w_out, seq_lengths):
    rows, width = hidden.shape
    zh, x, co, y, zl = (lax.axis_index(a) for a in ALL)
    mine = (zh * 4 + x) * 2 + co
    off = jnp.array([o % 4 for o in OFFSETS], jnp.int32)
    src_z, src_x = (zh + off) % 4, (x + off) % 4
    src_c = jnp.stack([co, 1 - co])
    all_4 = jnp.arange(4, dtype=jnp.int32)

    def table(x_at, z_at):
        places = z_at[None, None, :] * 8 + x_at[None, :, None] * 2 + src_c[:, None, None]
        return places.reshape(32).astype(jnp.int32)

    q_order, kv_order, block_order = table(src_x, src_z), table(all_4, all_4), table(src_x, all_4)

    moves = []
    for d in range(256):
        l = d % 2
        yy = d // 2 % 4
        c = d // 8 % 2
        xx = d // 16 % 4
        zz = d // 64
        moves.append((d, (((zz * 4 + (xx + yy) % 4) * 2 + l) * 4 + xx) * 2 + c))
    pick_key = zl == 0
    at = y * HEAD
    kv_block = jnp.where(
        pick_key,
        lax.dynamic_slice_in_dim(w_key, at, HEAD, 1),
        lax.dynamic_slice_in_dim(w_value, at, HEAD, 1),
    )
    kv_bias = jnp.where(
        pick_key,
        lax.dynamic_slice_in_dim(bias_key, at, HEAD, 0),
        lax.dynamic_slice_in_dim(bias_value, at, HEAD, 0),
    )
    kv_stack = spread(spread(kv_block, "zh", 4), "x", 4).reshape(16, -1, HEAD)
    kv_weights = both_cores([kv_stack])
    q_stack = jnp.stack(ring_gather(w_query, "zh"))
    q_weights = both_cores(ring_gather(q_stack, "x"))
    out_block = lax.ppermute(w_out, ALL, moves)
    out_stack = jnp.stack(ring_gather(out_block, "zh"))
    out_weights = both_cores(ring_gather(out_stack, "x"))

    ends = jnp.cumsum(seq_lengths)
    index = mine * rows + jnp.arange(rows, dtype=jnp.int32)
    begin = jnp.max(jnp.where(index[:, None] >= ends[None, :], ends[None, :], 0), axis=1).astype(jnp.int32)
    position = (index - begin).astype(F32)
    frequency = jnp.exp(jnp.arange(HEAD // 2, dtype=F32) * (-2.0 * math.log(ROPE_BASE) / HEAD))
    angle = position[:, None] * frequency[None, :]
    cos, sin = jnp.cos(angle), jnp.sin(angle)
    cos = jnp.concatenate([cos, cos], axis=1)
    sin = jnp.concatenate([-sin, sin], axis=1)
    kv_cos = jnp.where(pick_key, cos, 1.0)
    kv_sin = jnp.where(pick_key, sin, 0.0)

    def project(pieces, order, bias, cos, sin, base=0):
        cols = bias.shape[0]
        return call(
            functools.partial(project_kernel, [p[:3] for p in pieces], base),
            jax.ShapeDtypeStruct((rows, cols), BF16),
            (
                order,
                hidden,
                norm_gain[None, :],
                bias.astype(F32)[None, :],
                cos,
                sin,
                *[p[3] for p in pieces],
            ),
            scratch=[pltpu.VMEM((rows, width), BF16)],
            smem_count=1,
            extra=rows * width * 2,
            flops=2 * rows * width * cols,
            moved=2 * width * (rows + cols),
        )

    kv_own = project(kv_weights, kv_order, kv_bias, kv_cos, kv_sin)
    kv_other = swap(kv_own, "zl")
    kv_pair = jnp.concatenate(
        [jnp.where(pick_key, kv_own, kv_other), jnp.where(pick_key, kv_other, kv_own)], axis=1
    )
    kv_stack = spread(kv_pair, "zh", 4)
    kv = both_cores(ring_gather(kv_stack, "x"))
    row_of = ((src_x - y) % 4)[None, :] * 2 + src_c[:, None]
    info = jnp.stack([mine, begin[0] // rows, (begin[rows - 1] + rows - 1) // rows])
    tables = jnp.concatenate([block_order, q_order, row_of.reshape(8), src_z, info]).astype(jnp.int32)
    tables = pl.pallas_call(
        row_kernel,
        out_shape=jax.ShapeDtypeStruct(tables.shape, jnp.int32),
        in_specs=smem(1),
        out_specs=smem(1)[0],
        name="row",
    )(tables)
    query = project(q_weights, tables, bias_query, cos, sin, Q_ORDER)
    heads = query.shape[1] // HEAD
    attended = call(
        functools.partial(attend_kernel, [p[:3] for p in kv]),
        jax.ShapeDtypeStruct(query.shape, BF16),
        (tables, query, begin[None, :], *[p[3] for p in kv]),
        scratch=[
            pltpu.VMEM((34, rows, HEAD), BF16),
            pltpu.VMEM((34, HEAD, rows), BF16),
            pltpu.SMEM((34,), jnp.int32),
            pltpu.VMEM((2, 2 * rows, rows), F32),
            pltpu.VMEM((1, heads * rows), F32),
            pltpu.VMEM((1, heads * rows), F32),
            pltpu.VMEM((HEAD, heads * rows), F32),
        ],
        smem_count=1,
        extra=10 << 20,
        flops=4 * heads * rows * 6144 * HEAD * 2,
        moved=5 * 1024 * 1024,
        transcendentals=heads * rows * 6144,
    )

    parts = spread(attended, TP, 8)
    cols = width // 8
    mixed = call(
        functools.partial(output_kernel, [p[:2] for p in out_weights]),
        jax.ShapeDtypeStruct((rows, cols), BF16),
        (tables, parts, *[p[3] for p in out_weights]),
        smem_count=1,
        extra=38 << 20,
        flops=2 * rows * cols * 4096,
        moved=12 * 1024 * 1024,
    )
    share = rows // 8
    landed = lax.all_to_all(mixed.reshape(8, share, cols), TP, 0, 0, tiled=True)
    own = lax.dynamic_slice_in_dim(hidden, (y * 2 + zl) * share, share, 0)
    return call(
        finish_kernel,
        jax.ShapeDtypeStruct((share, width), F32),
        (own, landed),
        flops=2 * share * width,
        moved=8 * share * width,
    )


def solution(mesh):
    fine = Mesh(mesh.devices.reshape(4, 4, 2, 4, 2), ALL)

    return jax.shard_map(
        shards,
        mesh=fine,
        in_specs=(
            P(FSDP, None),
            P(),
            P(FSDP, TP),
            P(FSDP, None),
            P(FSDP, None),
            P(TP),
            P(),
            P(),
            P(TP, FSDP),
            P(),
        ),
        out_specs=P(ALL, None),
        check_vma=False,
    )
```
